128 devices in a mesh: dp: 8 (over z_lo, y), tensor: 16 (over z_hi, x, core).
Axes of the slice: x: 4, y: 4, z: 4 (z_hi: 2, z_lo: 2; z = z_hi * 2 + z_lo), core: 2. Of those that a mesh axis runs over, the one named last changes fastest.
Arguments:
- token_ids: int32 [4096], P('dp'), may hold values from 0 to 76031
- positions: int32 [4096], P('dp'), may hold values from 0 to 511, as said below
- embed_table: bfloat16 [76032, 8192], P('dp', 'tensor'), may hold values from -6 to 6
- norm_gain: float32 [8192], replicated, may hold values from 0.25 to 1.75
- wq: bfloat16 [8192, 8192], P(('dp', 'tensor')), may hold values from -1 to 1, as said below
- wk: bfloat16 [8192, 1024], P(('dp', 'tensor')), may hold values from -8 to 8, as said below
- wv: bfloat16 [8192, 1024], P(('dp', 'tensor')), may hold values from -0.0625 to 0.0625
Outputs:
- attended: bfloat16 [4096, 8192], P('dp', 'tensor')
The draws below stay inside these ranges and needn't reach their ends.
Inputs may be any that keep to these rules, and one draw needn't show every extreme that they name: `positions`: a position is 0 exactly where a prompt starts and otherwise one more than the previous token's; the first token of each block of 512 starts a prompt; in some block a single prompt fills all 512 tokens. `wq`: a weight matrix. `wk`: a weight matrix.
All inputs are finite; a program needn't handle non-finite values.
Results may differ from the reference program's by a relative error of at most 0.0025.
The reference program's roundings to bfloat16 on the way count: a program that leaves them out, or rounds other values in their place, can miss the bound.
Values may be sent and summed in bfloat16 or wider, within the bound.
A program may use at most 128 MiB of HBM per device.

```python
import math
import jax
import jax.numpy as jnp
import numpy as np
from jax import lax

MODEL_DIM = 8192
QUERY_HEADS = 64
KEY_VALUE_HEADS = 8
HEAD_SIZE = 128
VOCAB = 76032
GROUP_TOKENS = 512
ALL_TOKENS = 4096
N_DP = 8


def projection_pair(key):
    query_key = jax.random.fold_in(key, 101)
    key_dict_name = jax.random.fold_in(key, 202)
    query_matrix = jax.random.truncated_normal(query_key, -6.0, 6.0, (MODEL_DIM, QUERY_HEADS * HEAD_SIZE), jnp.float32) * MODEL_DIM ** (-0.5)
    key_matrix = jax.random.truncated_normal(key_dict_name, -6.0, 6.0, (MODEL_DIM, KEY_VALUE_HEADS * HEAD_SIZE), jnp.float32) * MODEL_DIM ** (-0.5)
    return (query_matrix, key_matrix)


def draw_wq(key, part):
    return projection_pair(key)[0].astype(jnp.bfloat16)


def draw_wk(key, part):
    return projection_pair(key)[1].astype(jnp.bfloat16)


def draw_positions(key, part):
    places = jnp.arange(ALL_TOKENS, dtype=jnp.int32)
    within = places % GROUP_TOKENS
    block_number = places // GROUP_TOKENS
    random_starts = (jax.random.randint(key, (ALL_TOKENS,), 0, 40) == 0) & (block_number != ALL_TOKENS // GROUP_TOKENS - 1)
    starts = random_starts | (within == 0)
    begin_at = lax.cummax(jnp.where(starts, places, 0), axis=0)
    return (places - begin_at).astype(jnp.int32)


def touch_ends(result, own_key, low, high):
    dims = result.shape
    spot = [jax.random.randint(jax.random.fold_in(own_key, axis), (), 0, dims[axis]) for axis in range(len(dims))]
    result = result.at[tuple(spot)].set(low)
    longest = dims.index(max(dims))
    spot[longest] = (spot[longest] + 1) % dims[longest]
    return result.at[tuple(spot)].set(high)


def levels(stream_key, shape, pieces, smallest, top_value):
    loudness = 1.0
    for position, parts in pieces:
        heights = jax.random.uniform(jax.random.fold_in(jax.random.fold_in(stream_key, 6), position), (parts,), jnp.float32, smallest / len(pieces), top_value / len(pieces))
        loudness = loudness * jnp.repeat(jnp.exp(heights), shape[position] // parts).reshape((-1,) + (1,) * (len(shape) - 1 - position))
    return loudness


def ranked_wide(rng, dims, count, skew):
    weights = [min(1 << octave, count + 1 - (1 << octave)) * (1 << 20) // math.isqrt((1 << octave) ** skew) + 1 for octave in range((count + 1).bit_length()) if 1 << octave <= count]
    scale = 1 + sum(weights) // (1 << 30)
    grid = np.cumsum(np.array([max(1, weight // scale) for weight in weights]))
    lot = jax.random.randint(jax.random.fold_in(rng, 1), dims, 0, int(grid[len(weights) - 1]))
    start = jnp.left_shift(1, jnp.searchsorted(jnp.asarray(grid, jnp.int32), lot, side="right").astype(jnp.int32))
    grade = start - 1 + jax.random.randint(jax.random.fold_in(rng, 4), dims, 0, 1 << 30) % jnp.minimum(start, count + 1 - start)
    return jax.random.permutation(jax.random.fold_in(rng, 2), count)[grade].astype(jnp.int32)


def gaussian(own_key, shape, spread, bound, cuts=(), kind=jnp.bfloat16):
    loudness = levels(own_key, shape, cuts, -0.22, 0.18) if cuts else 1.0
    entries = jax.random.normal(own_key, shape, jnp.float32) * spread * loudness
    return jnp.minimum(jnp.maximum(entries, -bound), bound).astype(kind)


def setup_inputs(seed: int = 0) -> dict:
    splits = jax.random.split(jax.random.key(seed), 8)
    token_ids = touch_ends(ranked_wide(splits[0], (ALL_TOKENS,), VOCAB, 2), jax.random.fold_in(splits[0], 3), 0, VOCAB - 1).astype(jnp.int32)
    positions = draw_positions(jax.random.fold_in(splits[7], 71), 0)
    embed_table = gaussian(splits[2], (VOCAB, MODEL_DIM), 1.0, 6.0, ((0, 8), (1, 16)))
    norm_gain = jnp.clip(1.0 + 0.15 * jax.random.normal(splits[3], (MODEL_DIM,), jnp.float32), 0.25, 1.75)
    wq = draw_wq(jax.random.fold_in(splits[7], 71), 0)
    wk = draw_wk(jax.random.fold_in(splits[7], 71), 0)
    wv = gaussian(splits[6], (MODEL_DIM, KEY_VALUE_HEADS * HEAD_SIZE), MODEL_DIM ** -0.5, 0.0625, ((0, 128),))
    return {"token_ids": token_ids, "positions": positions, "embed_table": embed_table, "norm_gain": norm_gain, "wq": wq, "wk": wk, "wv": wv}


def rotate(vectors, positions):
    half_dim = vectors.shape[-1] // 2
    frequency = 1000000.0 ** (-(jnp.arange(half_dim, dtype=jnp.float32) * 2.0 / vectors.shape[-1]))
    angles = positions.astype(jnp.float32)[:, None] * frequency[None, :]
    cosine = jnp.cos(angles)[:, None, :]
    sine_term = jnp.sin(angles)[:, None, :]
    lower_half = vectors[..., :half_dim]
    upper_half = vectors[..., half_dim:]
    return jnp.concatenate([lower_half * cosine - upper_half * sine_term, upper_half * cosine + lower_half * sine_term], axis=-1)

def reference(token_ids, positions, embed_table, norm_gain, wq, wk, wv):
    embedded = jnp.take(embed_table, token_ids, axis=0)
    hidden = embedded.astype(jnp.float32)
    mean_square = lax.optimization_barrier(jnp.mean(hidden * hidden, axis=-1, keepdims=True))
    normed_hidden = (hidden * lax.rsqrt(mean_square + 1e-06) * norm_gain.astype(jnp.float32)[None, :]).astype(jnp.bfloat16)
    query_raw = jnp.dot(normed_hidden, wq, preferred_element_type=jnp.float32).reshape(ALL_TOKENS, QUERY_HEADS, HEAD_SIZE)
    key_unnormed = jnp.dot(normed_hidden, wk, preferred_element_type=jnp.float32).reshape(ALL_TOKENS, KEY_VALUE_HEADS, HEAD_SIZE)
    value_unnormed = jnp.dot(normed_hidden, wv, preferred_element_type=jnp.float32).reshape(ALL_TOKENS, KEY_VALUE_HEADS, HEAD_SIZE)
    query_tensor = rotate(query_raw, positions).astype(jnp.bfloat16)
    key_row_block = rotate(key_unnormed, positions).astype(jnp.bfloat16)
    value_tensor = value_unnormed.astype(jnp.bfloat16)
    scale = 1.0 / HEAD_SIZE ** 0.5

    def attend_rollout_group(packed):
        group_query, rollout_keys, rollout_values, group_positions = packed
        key_head_tensor = jnp.repeat(rollout_keys, QUERY_HEADS // KEY_VALUE_HEADS, axis=1).astype(jnp.float32)
        value_head_tensor = jnp.repeat(rollout_values, QUERY_HEADS // KEY_VALUE_HEADS, axis=1).astype(jnp.float32)
        scores = jnp.einsum('qhd,khd->hqk', group_query.astype(jnp.float32), key_head_tensor) * scale
        places = jnp.arange(GROUP_TOKENS, dtype=jnp.int32)
        allowed = (places[None, :] <= places[:, None]) & (group_positions[:, None] - group_positions[None, :] == places[:, None] - places[None, :])
        scores = jnp.where(allowed[None, :, :], scores, -1e+30)
        largest = lax.optimization_barrier(jnp.max(scores, axis=-1, keepdims=True))
        exponent = jnp.where(allowed[None, :, :], jnp.exp(scores - largest), 0.0)
        probs = (exponent / lax.optimization_barrier(jnp.sum(exponent, axis=-1, keepdims=True))).astype(jnp.bfloat16)
        output = jnp.einsum('hqk,khd->qhd', probs.astype(jnp.float32), value_head_tensor)
        return output.astype(jnp.bfloat16)
    attended = lax.map(attend_rollout_group, (query_tensor.reshape(N_DP, GROUP_TOKENS, QUERY_HEADS, HEAD_SIZE), key_row_block.reshape(N_DP, GROUP_TOKENS, KEY_VALUE_HEADS, HEAD_SIZE), value_tensor.reshape(N_DP, GROUP_TOKENS, KEY_VALUE_HEADS, HEAD_SIZE), positions.reshape(N_DP, GROUP_TOKENS)))
    return attended.reshape(ALL_TOKENS, QUERY_HEADS * HEAD_SIZE)
```

```python
import jax
import jax.numpy as jnp
from jax import lax
from jax.experimental import pallas as pl
from jax.experimental.pallas import tpu as pltpu
from jax.sharding import PartitionSpec as P

MESH = pl.DeviceIdType.MESH
F32, BF16, I32 = jnp.float32, jnp.bfloat16, jnp.int32
TOK = 512
PART = 256
ROWS = 9504
HEAD = 128
TAB_COPIES = 6
NEG = -1e30


def kernel(
    ids, cosine, sine, first_col, first_row, gain, table, wq, wk, wv, out,
    landed, tab, stage, ids_all, index_v, index_s, mine, half_in, final_in,
    zsend, zrecv, acts, normed, wa, wb, psa, pra, psb, prb, acca, accb, kv,
    sq, sq_own, sq_in, inv,
    ids_ss, ids_rs, tab_sem, sm_sem, x_ss, x_rs, g_ss, h_rs, f_rs, z_ss, z_rs,
    a_ss, a_rs, q_ss, q_rs, w_ss, wa_rs, wb_rs, p_ss, p_rs, kv_ss, kv_rs,
):
    d = lax.axis_index("dp")
    t = lax.axis_index("tensor")
    zl, y = d // 4, lax.rem(d, 4)
    h, x, k = t // 8, lax.rem(t // 2, 4), lax.rem(t, 2)
    yp, y2, ym = lax.rem(y + 1, 4), lax.rem(y + 2, 4), lax.rem(y + 3, 4)
    xp, x2, xm = lax.rem(x + 1, 4), lax.rem(x + 2, 4), lax.rem(x + 3, 4)
    up, down, over = (zl * 4 + yp, t), (zl * 4 + ym, t), ((1 - zl) * 4 + y, t)

    def slot(hh, xx, kk):
        return hh * 8 + xx * 2 + kk

    started = []

    def send(src, dst, ss, rs, device):
        copy = pltpu.make_async_remote_copy(
            src_ref=src, dst_ref=dst, send_sem=ss, recv_sem=rs, device_id=device, device_id_type=MESH
        )
        copy.start()
        started.append(copy)

    def arrived(dst, ss, rs):
        pltpu.make_async_remote_copy(
            src_ref=dst, dst_ref=dst, send_sem=ss, recv_sem=rs, device_id=over, device_id_type=MESH
        ).wait_recv()

    part = ROWS // TAB_COPIES

    def load(i):
        return pltpu.make_async_copy(
            table.at[pl.ds(i * part, part)], landed.at[i % 3], tab_sem.at[i]
        )

    def widen(i):
        load(i).wait()

        def body(n, _):
            at = pl.multiple_of(n * 48, 16)
            tab[pl.ds(pl.multiple_of(i * part + n * 48, 16), 48), :] = landed[
                i % 3, pl.ds(at, 48), :
            ].astype(F32)
            return 0

        lax.fori_loop(0, part // 48, body, 0)
        if i + 3 < TAB_COPIES:
            load(i + 3).start()

    for i in range(3):
        load(i).start()

    barrier = pltpu.get_barrier_semaphore()

    def greet_plane(i, _):
        dd = lax.rem(zl + i // 16, 2) * 4 + y
        tt = lax.rem(t + i, 16)
        pl.semaphore_signal(barrier, inc=1, device_id=(dd, tt), device_id_type=MESH)
        return 0

    lax.fori_loop(1, 32, greet_plane, 0)

    def greet_row(i, _):
        dd = lax.rem(zl + i // 3, 2) * 4 + lax.rem(y + 1 + lax.rem(i, 3), 4)
        pl.semaphore_signal(barrier, inc=1, device_id=(dd, t), device_id_type=MESH)
        return 0

    lax.fori_loop(0, 6, greet_row, 0)
    tab[pl.ds(ROWS, 8), :] = jnp.zeros((8, 512), F32)
    widen(0)
    pl.semaphore_wait(barrier, 37)

    for i in range(1, 8):
        send(ids.at[0], ids_all.at[d], ids_ss.at[i - 1], ids_rs.at[i - 1], (lax.rem(d + i, 8), t))

    row = pl.multiple_of(((zl * 2 + h) * 4 + lax.rem(x, 2) * 2 + k) * 64, 64)
    plane = x // 2

    def pieces(tt, wkv):
        q0 = pl.multiple_of(tt * 512, 256)
        c0 = pl.multiple_of((tt // 2) * HEAD, HEAD)
        return (
            (wkv.at[:, pl.ds(c0, HEAD)], wa.at[y, pl.ds(row, 64), pl.ds(0, HEAD)], 0),
            (wq.at[:, pl.ds(q0, 256)], wa.at[y, pl.ds(row, 64), pl.ds(HEAD, 256)], 0),
            (wq.at[:, pl.ds(pl.multiple_of(q0 + 256, 256), 256)], wb.at[y, pl.ds(row, 64), :], 1),
        )

    def outgoing(i, tt, wkv):
        return [
            pltpu.make_async_remote_copy(
                src_ref=src, dst_ref=dst, send_sem=x_ss.at[i, n], recv_sem=x_rs.at[r],
                device_id=(plane * 4 + y, tt), device_id_type=MESH,
            )
            for n, (src, dst, r) in enumerate(pieces(tt, wkv))
        ]

    def distribute(i, _):
        tt = lax.rem(t + i, 16)
        here = jnp.logical_and(i == 0, plane == zl)
        for core, wkv in ((0, wk), (1, wv)):
            turn = lax.rem(tt, 2) == core

            @pl.when(jnp.logical_and(turn, jnp.logical_not(here)))
            def _():
                for copy in outgoing(i, tt, wkv):
                    copy.start()

            @pl.when(jnp.logical_and(turn, here))
            def _():
                for src, dst, r in pieces(tt, wkv):
                    pltpu.make_async_copy(src, dst, x_rs.at[r]).start()

        return 0

    lax.fori_loop(0, 16, distribute, 0)

    for i in range(1, TAB_COPIES):
        widen(i)
    ids_all[d] = ids[0]
    for i in range(1, 8):
        arrived(ids_all.at[lax.rem(d + 8 - i, 8)], ids_ss.at[i - 1], ids_rs.at[i - 1])
    local = ids_all[...] - d * ROWS
    index_v[...] = jnp.where((local >= 0) & (local < ROWS), local, ROWS)
    to_scalar = pltpu.make_async_copy(index_v, index_s, sm_sem)
    to_scalar.start()
    to_scalar.wait()

    def gather(c, rel, g):
        group = g * 4 + lax.rem(y + rel, 4)

        def pick(i, _):
            line, first = c * 2 + i // 8, lax.rem(i, 8) * 16
            for j in range(16):
                stage[pl.ds(i * 16 + j, 1), :] = tab[pl.ds(index_s[group, line, first + j], 1), :]
            return 0

        lax.fori_loop(0, PART // 16, pick, 0)

        def narrow(i, _):
            rows = pl.ds(pl.multiple_of(i * 64, 64), 64)
            mine[c, rel, g, rows, :] = stage[rows, :].astype(BF16)
            return 0

        lax.fori_loop(0, PART // 64, narrow, 0)

    def first_sends(c):
        send(mine.at[c, 2, 0], half_in.at[c, 0], g_ss.at[c, 0], h_rs.at[c, 0], up)
        send(mine.at[c, 2, 1], half_in.at[c, 1], g_ss.at[c, 1], h_rs.at[c, 1], down)
        send(mine.at[c, 1, 1], final_in.at[c, 0, 1], g_ss.at[c, 2], f_rs.at[c, 0, 1], up)
        send(mine.at[c, 3, 0], final_in.at[c, 1, 0], g_ss.at[c, 3], f_rs.at[c, 1, 0], down)

    def second_sends(c):
        arrived(half_in.at[c, 0], g_ss.at[c, 0], h_rs.at[c, 0])
        mine[c, 1, 0] = mine[c, 1, 0] + half_in[c, 0]
        send(mine.at[c, 1, 0], final_in.at[c, 0, 0], g_ss.at[c, 4], f_rs.at[c, 0, 0], up)
        arrived(half_in.at[c, 1], g_ss.at[c, 1], h_rs.at[c, 1])
        mine[c, 3, 1] = mine[c, 3, 1] + half_in[c, 1]
        send(mine.at[c, 3, 1], final_in.at[c, 1, 1], g_ss.at[c, 5], f_rs.at[c, 1, 1], down)

    kept = pl.multiple_of(zl * 256, 256)
    given = pl.multiple_of((1 - zl) * 256, 256)

    def finish_rows(c):
        for g in range(2):
            for side in range(2):
                arrived(final_in.at[c, side, g], g_ss.at[c, 0], f_rs.at[c, side, g])
            rows = pl.ds(g * PART, PART)
            for at, to in ((given, None), (kept, t)):
                cols = pl.ds(at, 256)
                total = mine[c, 0, g, :, cols] + final_in[c, 0, g, :, cols] + final_in[c, 1, g, :, cols]
                if to is None:
                    zsend[c, rows, :] = total
                else:
                    acts[to, c, rows, :] = total
        send(zsend.at[c], zrecv.at[c], z_ss.at[c], z_rs.at[c], over)

    at_xp, at_xm = (d, slot(h, xp, k)), (d, slot(h, xm, k))
    at_z, at_core = (d, slot(1 - h, x, k)), (d, slot(h, x, 1 - k))

    def push(c, s, i, device):
        send(acts.at[s, c], acts.at[s, c], a_ss.at[c, i], a_rs.at[c, s], device)

    def have(c, s):
        arrived(acts.at[s, c], a_ss.at[c, 0], a_rs.at[c, s])

    def spread_own(c):
        arrived(zrecv.at[c], z_ss.at[c], z_rs.at[c])
        acts[t, c] = acts[t, c] + zrecv[c]
        push(c, t, 0, at_z)
        push(c, t, 1, at_xp)
        push(c, t, 2, at_xm)
        push(c, t, 3, at_core)

    def spread_near(c):
        s = slot(h, xm, k)
        have(c, s)
        push(c, s, 4, at_xp)
        push(c, s, 5, at_core)
        s = slot(h, xp, k)
        have(c, s)
        push(c, s, 6, at_core)

    def spread_far(c):
        s = slot(1 - h, x, k)
        have(c, s)
        push(c, s, 7, at_xp)
        push(c, s, 8, at_xm)
        push(c, s, 9, at_core)

    def spread_rest(c):
        s = slot(1 - h, xp, k)
        have(c, s)
        push(c, s, 10, at_xm)
        push(c, s, 11, at_core)
        s = slot(1 - h, xm, k)
        have(c, s)
        push(c, s, 12, at_core)
        for i in range(2):
            s = slot(i, x2, k)
            have(c, s)
            push(c, s, 13 + i, at_core)

    top, low = pl.ds(0, 512), pl.ds(512, 512)

    def pushw(ref, b, rows, i, rs, device):
        src = ref.at[b] if rows is None else ref.at[b, rows]
        send(src, src, w_ss.at[i], rs, device)

    def whole_weights(ref, r):
        pltpu.make_async_copy(ref.at[y], ref.at[y], x_rs.at[r]).wait()

    def first_weights():
        whole_weights(wa, 0)
        pushw(wa, y, None, 0, wa_rs.at[0], up)
        pushw(wa, y, None, 1, wa_rs.at[1], down)
        whole_weights(wb, 1)
        pushw(wb, y, top, 2, wb_rs.at[0], up)
        pushw(wb, y, low, 3, wb_rs.at[1], down)

    def relay_weights():
        arrived(wa.at[ym], w_ss.at[0], wa_rs.at[0])
        pushw(wa, ym, top, 4, wa_rs.at[2], up)
        arrived(wa.at[yp], w_ss.at[0], wa_rs.at[1])
        pushw(wa, yp, low, 5, wa_rs.at[3], down)
        pushw(wb, y, low, 6, wb_rs.at[4], up)
        pushw(wb, y, top, 7, wb_rs.at[5], down)

    def last_weights():
        arrived(wb.at[ym, top], w_ss.at[0], wb_rs.at[0])
        pushw(wb, ym, top, 8, wb_rs.at[2], up)
        arrived(wb.at[yp, low], w_ss.at[0], wb_rs.at[1])
        pushw(wb, yp, low, 9, wb_rs.at[3], down)

    def squares(c):
        for hh in range(2):
            for xx in range(4):
                have(c, slot(hh, xx, 1 - k))

        def body(i, _):
            rows = pl.ds(pl.multiple_of(i * 64, 64), 64)
            total = jnp.zeros((64, 128), F32)
            for s in range(16):
                v = acts[s, c, rows, :].astype(F32)
                v = v * v
                total = total + (v[:, :128] + v[:, 128:])
            sq[rows, :] = total
            return 0

        lax.fori_loop(0, 8, body, 0)
        for i in range(4):
            sq_own[c, i : i + 1, :] = jnp.sum(
                jnp.transpose(sq[i * 128 : (i + 1) * 128, :]), axis=0, keepdims=True
            )
        send(sq_own.at[c], sq_in.at[c], q_ss.at[c], q_rs.at[c], over)

    def norm(c):
        arrived(sq_in.at[c], q_ss.at[c], q_rs.at[c])
        for i in range(4):
            mean = (sq_own[c, i : i + 1, :] + sq_in[c, i : i + 1, :]) * (1.0 / 8192.0)
            inv[i * 128 : (i + 1) * 128, :] = jnp.transpose(
                jnp.broadcast_to(lax.rsqrt(mean + 1e-06), (128, 128))
            )

        def body(s, _):
            a, b, cc = s // 8, lax.rem(s // 2, 4), lax.rem(s, 2)
            at = pl.multiple_of(b * 1024 + (a * 2 + cc) * 256, 256)
            weight = gain[s * 2 + zl]
            for g in range(2):
                rows = pl.ds(g * PART, PART)
                scale = inv[rows, :]
                v = acts[s, c, rows, :].astype(F32)
                v = v * jnp.concatenate([scale, scale], axis=1) * weight
                normed[g, pl.ds(c * PART, PART), pl.ds(at, 256)] = v.astype(BF16)
            return 0

        lax.fori_loop(0, 16, body, 0)

    def project(g, w, acc, blocks, fresh):
        def body(i, _):
            b = lax.rem(y + blocks(i), 4)
            cols = pl.ds(pl.multiple_of(b * 1024, 1024), 1024)
            acc[...] += jnp.dot(normed[g, :, cols], w[b], preferred_element_type=F32)
            return 0

        if fresh:
            acc[...] = jnp.zeros_like(acc)
        lax.fori_loop(0, 4, body, 0)

    def rotate(v):
        return v * cosine[...] + pltpu.roll(v, 64, axis=1) * sine[...]

    def attend(query, head):
        for block in range(2):
            seen = (block + 1) * 256
            rows = slice(block * 256, seen)
            scores = lax.dot_general(
                query[rows], kv[0, :seen, :], (((1,), (1,)), ((), ())), preferred_element_type=F32
            ) * (1.0 / HEAD**0.5)
            i = lax.broadcasted_iota(I32, (256, seen), 0) + block * 256
            j = lax.broadcasted_iota(I32, (256, seen), 1)
            allowed = (j <= i) & (first_col[rows, :] == first_row[:, :seen])
            scores = jnp.where(allowed, scores, NEG)
            largest = jnp.max(scores, axis=-1, keepdims=True)
            weight = jnp.where(allowed, jnp.exp(scores - largest), 0.0)
            probs = (weight / jnp.sum(weight, axis=-1, keepdims=True)).astype(BF16)
            out[rows, head * HEAD : (head + 1) * HEAD] = jnp.dot(
                probs, kv[1, :seen, :], preferred_element_type=F32
            ).astype(BF16)

    gather(0, 2, 0)
    gather(0, 2, 1)
    gather(0, 1, 1)
    gather(0, 3, 0)
    first_sends(0)
    for rel, g in ((1, 0), (3, 1), (0, 0), (0, 1)):
        gather(0, rel, g)
    for rel, g in ((2, 0), (2, 1), (1, 1), (3, 0)):
        gather(1, rel, g)
    second_sends(0)
    first_sends(1)
    for rel, g in ((1, 0), (3, 1), (0, 0), (0, 1)):
        gather(1, rel, g)
    finish_rows(0)
    second_sends(1)
    spread_own(0)
    first_weights()
    finish_rows(1)
    spread_near(0)
    spread_far(0)
    spread_own(1)
    spread_rest(0)
    spread_near(1)
    relay_weights()
    spread_far(1)
    last_weights()
    squares(0)
    spread_rest(1)
    norm(0)
    squares(1)
    norm(1)

    own, other = zl, 1 - zl
    order = lambda i: i
    arrived(wa.at[y2, top], w_ss.at[0], wa_rs.at[2])
    arrived(wa.at[y2, low], w_ss.at[0], wa_rs.at[3])
    project(other, wa, acca, order, True)
    psa[...] = acca[...]
    send(psa, pra, p_ss.at[0], p_rs.at[0], over)
    project(own, wa, acca, order, True)
    arrived(pra, p_ss.at[0], p_rs.at[0])
    first = acca[:, 0:HEAD] + pra[:, 0:HEAD]
    kv[k] = jnp.where(k == 0, rotate(first), first).astype(BF16)
    send(kv.at[k], kv.at[k], kv_ss, kv_rs, at_core)
    arrived(kv.at[1 - k], kv_ss, kv_rs)
    for n in range(2):
        cols = slice((n + 1) * HEAD, (n + 2) * HEAD)
        attend(rotate(acca[:, cols] + pra[:, cols]).astype(BF16), n)

    arrived(wb.at[ym, low], w_ss.at[0], wb_rs.at[4])
    arrived(wb.at[yp, top], w_ss.at[0], wb_rs.at[5])
    arrived(wb.at[y2, top], w_ss.at[0], wb_rs.at[2])
    arrived(wb.at[y2, low], w_ss.at[0], wb_rs.at[3])
    project(other, wb, accb, order, True)
    psb[...] = accb[...]
    send(psb, prb, p_ss.at[1], p_rs.at[1], over)
    project(own, wb, accb, order, True)
    arrived(prb, p_ss.at[1], p_rs.at[1])
    for n in range(2):
        cols = slice(n * HEAD, (n + 1) * HEAD)
        attend(rotate(accb[:, cols] + prb[:, cols]).astype(BF16), 2 + n)

    for copy in started:
        copy.wait_send()

    def settle(i, _):
        tt = lax.rem(t + i, 16)

        @pl.when(jnp.logical_not(jnp.logical_and(i == 0, plane == zl)))
        def _():
            for copy in outgoing(i, tt, wk):
                copy.wait_send()

        return 0

    lax.fori_loop(0, 16, settle, 0)


def on_device(token_ids, positions, embed_table, norm_gain, wq, wk, wv):
    frequency = 1000000.0 ** (-(jnp.arange(64, dtype=F32) * 2.0 / HEAD))
    angles = positions.astype(F32)[:, None] * frequency[None, :]
    cosine, sine = jnp.cos(angles), jnp.sin(angles)
    first = jnp.arange(TOK, dtype=I32) - positions
    vmem = pl.BlockSpec(memory_space=pltpu.VMEM)
    far = pl.BlockSpec(memory_space=pl.ANY)
    dma = pltpu.SemaphoreType.DMA
    return pl.pallas_call(
        kernel,
        out_shape=jax.ShapeDtypeStruct((TOK, 512), BF16),
        in_specs=[vmem] * 6 + [far] * 4,
        out_specs=vmem,
        scratch_shapes=[
            pltpu.VMEM((3, ROWS // TAB_COPIES, 512), BF16),
            pltpu.VMEM((ROWS + 8, 512), F32),
            pltpu.VMEM((PART, 512), F32),
            pltpu.VMEM((8, 4, 128), I32),
            pltpu.VMEM((8, 4, 128), I32),
            pltpu.SMEM((8, 4, 128), I32),
            pltpu.VMEM((2, 4, 2, PART, 512), BF16),
            pltpu.VMEM((2, 2, PART, 512), BF16),
            pltpu.VMEM((2, 2, 2, PART, 512), BF16),
            pltpu.VMEM((2, 512, 256), BF16),
            pltpu.VMEM((2, 512, 256), BF16),
            pltpu.VMEM((16, 2, 512, 256), BF16),
            pltpu.VMEM((2, 512, 4096), BF16),
            pltpu.VMEM((4, 1024, 384), BF16),
            pltpu.VMEM((4, 1024, 256), BF16),
            pltpu.VMEM((TOK, 384), F32),
            pltpu.VMEM((TOK, 384), F32),
            pltpu.VMEM((TOK, 256), F32),
            pltpu.VMEM((TOK, 256), F32),
            pltpu.VMEM((TOK, 384), F32),
            pltpu.VMEM((TOK, 256), F32),
            pltpu.VMEM((2, TOK, HEAD), BF16),
            pltpu.VMEM((512, 128), F32),
            pltpu.VMEM((2, 4, 128), F32),
            pltpu.VMEM((2, 4, 128), F32),
            pltpu.VMEM((512, 128), F32),
            dma((7,)), dma((7,)), dma((TAB_COPIES,)), dma,
            dma((16, 3)), dma((2,)),
            dma((2, 6)), dma((2, 2)), dma((2, 2, 2)),
            dma((2,)), dma((2,)),
            dma((2, 15)), dma((2, 16)),
            dma((2,)), dma((2,)),
            dma((10,)), dma((4,)), dma((6,)),
            dma((2,)), dma((2,)),
            dma, dma,
        ],
        compiler_params=pltpu.CompilerParams(
            collective_id=0, has_side_effects=True, vmem_limit_bytes=63 * 2**20
        ),
    )(
        token_ids.reshape(1, 4, 128),
        jnp.concatenate([cosine, cosine], axis=1),
        jnp.concatenate([-sine, sine], axis=1),
        first.reshape(TOK, 1),
        first.reshape(1, TOK),
        norm_gain.reshape(32, 1, 256),
        embed_table,
        wq,
        wk,
        wv,
    )


def solution(mesh):
    split = P(("dp", "tensor"), None)
    return jax.shard_map(
        on_device,
        mesh=mesh,
        in_specs=(P("dp"), P("dp"), P("dp", "tensor"), P(), split, split, split),
        out_specs=P("dp", "tensor"),
        check_vma=False,
    )
```

```python
import jax
import jax.numpy as jnp
from jax import lax
from jax.experimental import pallas as pl
from jax.experimental.pallas import tpu as pltpu
from jax.sharding import PartitionSpec as P

MESH = pl.DeviceIdType.MESH
F32, BF16, I32 = jnp.float32, jnp.bfloat16, jnp.int32
TOK = 512
PART = 128
CHUNKS = TOK // PART
SPLIT = 2
BAND = TOK // SPLIT
PIECES = 5
ROWS = 9504
HEAD = 128
TAB_COPIES = 6
NEG = -1e30


def kernel(
    ids, place, frequency, gain, table, wq, wk, wv, out,
    landed, tab, stage, ids_all, index_v, index_s, mine, half_in, final_in,
    zsend, zrecv, acts, normed, weights, psend, precv, kept_sum, kv,
    sq, sq_own, sq_in, inv, cosine, sine, first_col,
    ids_ss, ids_rs, tab_sem, sm_sem, x_ss, x_rs, g_ss, h_rs, f_rs, z_ss, z_rs,
    a_ss, a_rs, q_ss, q_rs, w_ss, w_rs, p_ss, p_rs, kv_ss, kv_rs,
):
    d = lax.axis_index("dp")
    t = lax.axis_index("tensor")
    zl, y = d // 4, lax.rem(d, 4)
    h, x, k = t // 8, lax.rem(t // 2, 4), lax.rem(t, 2)
    yp, y2, ym = lax.rem(y + 1, 4), lax.rem(y + 2, 4), lax.rem(y + 3, 4)
    xp, x2, xm = lax.rem(x + 1, 4), lax.rem(x + 2, 4), lax.rem(x + 3, 4)
    up, down, over = (zl * 4 + yp, t), (zl * 4 + ym, t), ((1 - zl) * 4 + y, t)

    def slot(hh, xx, kk):
        return hh * 8 + xx * 2 + kk

    started = []

    def send(src, dst, ss, rs, device):
        copy = pltpu.make_async_remote_copy(
            src_ref=src, dst_ref=dst, send_sem=ss, recv_sem=rs, device_id=device, device_id_type=MESH
        )
        copy.start()
        started.append(copy)

    def arrived(dst, ss, rs):
        pltpu.make_async_remote_copy(
            src_ref=dst, dst_ref=dst, send_sem=ss, recv_sem=rs, device_id=over, device_id_type=MESH
        ).wait_recv()

    part = ROWS // TAB_COPIES

    def load(i):
        return pltpu.make_async_copy(
            table.at[pl.ds(i * part, part)], landed.at[i % 3], tab_sem.at[i]
        )

    def widen(i):
        load(i).wait()

        def body(n, _):
            at = pl.multiple_of(n * 48, 16)
            tab[pl.ds(pl.multiple_of(i * part + n * 48, 16), 48), :] = landed[
                i % 3, pl.ds(at, 48), :
            ].astype(F32)
            return 0

        lax.fori_loop(0, part // 48, body, 0)
        if i + 3 < TAB_COPIES:
            load(i + 3).start()

    for i in range(3):
        load(i).start()

    barrier = pltpu.get_barrier_semaphore()

    def greet_plane(i, _):
        dd = lax.rem(zl + i // 16, 2) * 4 + y
        tt = lax.rem(t + i, 16)
        pl.semaphore_signal(barrier, inc=1, device_id=(dd, tt), device_id_type=MESH)
        return 0

    lax.fori_loop(1, 32, greet_plane, 0)

    def greet_row(i, _):
        dd = lax.rem(zl + i // 3, 2) * 4 + lax.rem(y + 1 + lax.rem(i, 3), 4)
        pl.semaphore_signal(barrier, inc=1, device_id=(dd, t), device_id_type=MESH)
        return 0

    lax.fori_loop(0, 6, greet_row, 0)
    pl.semaphore_wait(barrier, 37)

    for i in range(1, 8):
        send(ids.at[0], ids_all.at[d], ids_ss.at[i - 1], ids_rs.at[i - 1], (lax.rem(d + i, 8), t))

    tab[pl.ds(ROWS, 8), :] = jnp.zeros((8, 512), F32)
    for i in range(TAB_COPIES):
        widen(i)

    row = pl.multiple_of(((zl * 2 + h) * 4 + lax.rem(x, 2) * 2 + k) * 64, 64)
    plane = x // 2

    def pieces(tt, wkv):
        q0 = pl.multiple_of(tt * 512, 256)
        c0 = pl.multiple_of((tt // 2) * HEAD, HEAD)
        to = [weights.at[j, y, pl.ds(row, 64), :] for j in range(PIECES)]
        return [(wkv.at[:, pl.ds(c0, HEAD)], to[0], 0)] + [
            (wq.at[:, pl.ds(pl.multiple_of(q0 + n * HEAD, HEAD), HEAD)], to[n + 1], n + 1)
            for n in range(4)
        ]

    def outgoing(i, tt, wkv):
        return [
            pltpu.make_async_remote_copy(
                src_ref=src, dst_ref=dst, send_sem=x_ss.at[i, n], recv_sem=x_rs.at[r],
                device_id=(plane * 4 + y, tt), device_id_type=MESH,
            )
            for n, (src, dst, r) in enumerate(pieces(tt, wkv))
        ]

    def distribute(i, _):
        tt = lax.rem(t + i, 16)
        here = jnp.logical_and(i == 0, plane == zl)
        for core, wkv in ((0, wk), (1, wv)):
            turn = lax.rem(tt, 2) == core

            @pl.when(jnp.logical_and(turn, jnp.logical_not(here)))
            def _():
                for copy in outgoing(i, tt, wkv):
                    copy.start()

            @pl.when(jnp.logical_and(turn, here))
            def _():
                for src, dst, r in pieces(tt, wkv):
                    pltpu.make_async_copy(src, dst, x_rs.at[r]).start()

        return 0

    def distribute_all():
        lax.fori_loop(0, 16, distribute, 0)

    ids_all[d] = ids[0]
    for i in range(1, 8):
        arrived(ids_all.at[lax.rem(d + 8 - i, 8)], ids_ss.at[i - 1], ids_rs.at[i - 1])
    local = ids_all[...] - d * ROWS
    index_v[...] = jnp.where((local >= 0) & (local < ROWS), local, ROWS)
    to_scalar = pltpu.make_async_copy(index_v, index_s, sm_sem)
    to_scalar.start()
    to_scalar.wait()

    def gather(c, rel, g):
        group = g * 4 + lax.rem(y + rel, 4)

        def pick(i, _):
            for j in range(16):
                stage[pl.ds(i * 16 + j, 1), :] = tab[pl.ds(index_s[group, c, i * 16 + j], 1), :]
            return 0

        lax.fori_loop(0, PART // 16, pick, 0)

        def narrow(i, _):
            rows = pl.ds(pl.multiple_of(i * 64, 64), 64)
            mine[c, rel, g, rows, :] = stage[rows, :].astype(BF16)
            return 0

        lax.fori_loop(0, PART // 64, narrow, 0)

    def rows_a(c):
        for g, to in ((0, up), (1, down)):
            gather(c, 2, g)
            send(mine.at[c, 2, g], half_in.at[c, g], g_ss.at[c, g], h_rs.at[c, g], to)

    def rows_b(c):
        gather(c, 1, 1)
        send(mine.at[c, 1, 1], final_in.at[c, 0, 1], g_ss.at[c, 2], f_rs.at[c, 0, 1], up)
        gather(c, 3, 0)
        send(mine.at[c, 3, 0], final_in.at[c, 1, 0], g_ss.at[c, 3], f_rs.at[c, 1, 0], down)

    def rows_own(c):
        for rel, g in ((1, 0), (3, 1), (0, 0), (0, 1)):
            gather(c, rel, g)

    def rows_c(c):
        arrived(half_in.at[c, 0], g_ss.at[c, 0], h_rs.at[c, 0])
        mine[c, 1, 0] = mine[c, 1, 0] + half_in[c, 0]
        send(mine.at[c, 1, 0], final_in.at[c, 0, 0], g_ss.at[c, 4], f_rs.at[c, 0, 0], up)
        arrived(half_in.at[c, 1], g_ss.at[c, 1], h_rs.at[c, 1])
        mine[c, 3, 1] = mine[c, 3, 1] + half_in[c, 1]
        send(mine.at[c, 3, 1], final_in.at[c, 1, 1], g_ss.at[c, 5], f_rs.at[c, 1, 1], down)

    kept = pl.multiple_of(zl * 256, 256)
    given = pl.multiple_of((1 - zl) * 256, 256)

    def finish_rows(c):
        for g in range(2):
            for side in range(2):
                arrived(final_in.at[c, side, g], g_ss.at[c, 0], f_rs.at[c, side, g])
            rows = pl.ds(g * PART, PART)
            for at, to in ((given, None), (kept, t)):
                cols = pl.ds(at, 256)
                total = mine[c, 0, g, :, cols] + final_in[c, 0, g, :, cols] + final_in[c, 1, g, :, cols]
                if to is None:
                    zsend[c, rows, :] = total
                else:
                    acts[to, c, rows, :] = total
        send(zsend.at[c], zrecv.at[c], z_ss.at[c], z_rs.at[c], over)

    at_xp, at_xm = (d, slot(h, xp, k)), (d, slot(h, xm, k))
    at_z, at_core = (d, slot(1 - h, x, k)), (d, slot(h, x, 1 - k))

    def push(c, s, i, device):
        send(acts.at[s, c], acts.at[s, c], a_ss.at[c, i], a_rs.at[c, s], device)

    def have(c, s):
        arrived(acts.at[s, c], a_ss.at[c, 0], a_rs.at[c, s])

    def spread_own(c):
        arrived(zrecv.at[c], z_ss.at[c], z_rs.at[c])
        acts[t, c] = acts[t, c] + zrecv[c]
        push(c, t, 0, at_z)
        push(c, t, 1, at_xp)
        push(c, t, 2, at_xm)
        push(c, t, 3, at_core)

    def spread_near(c):
        s = slot(h, xm, k)
        have(c, s)
        push(c, s, 4, at_xp)
        push(c, s, 5, at_core)

    def spread_far(c):
        s = slot(1 - h, x, k)
        have(c, s)
        push(c, s, 7, at_xm)
        push(c, s, 8, at_xp)
        push(c, s, 9, at_core)

    def spread_pass(c):
        s = slot(1 - h, xp, k)
        have(c, s)
        push(c, s, 10, at_xm)
        push(c, s, 11, at_core)

    def spread_rest(c):
        for i, s in (
            (6, slot(h, xp, k)), (12, slot(1 - h, xm, k)), (13, slot(0, x2, k)), (14, slot(1, x2, k)),
        ):
            have(c, s)
            push(c, s, i, at_core)

    top, low = pl.ds(0, 512), pl.ds(512, 512)

    def weights_own(j):
        src = weights.at[j, y]
        pltpu.make_async_copy(src, src, x_rs.at[j]).wait()
        send(src, src, w_ss.at[j, 0], w_rs.at[j, 0], up)
        send(src, src, w_ss.at[j, 1], w_rs.at[j, 1], down)

    def weights_pass(j):
        arrived(weights.at[j, ym], w_ss.at[j, 0], w_rs.at[j, 0])
        src = weights.at[j, ym, top]
        send(src, src, w_ss.at[j, 2], w_rs.at[j, 2], up)
        arrived(weights.at[j, yp], w_ss.at[j, 0], w_rs.at[j, 1])
        src = weights.at[j, yp, low]
        send(src, src, w_ss.at[j, 3], w_rs.at[j, 3], down)

    def weights_whole(j):
        arrived(weights.at[j, y2, top], w_ss.at[j, 0], w_rs.at[j, 2])
        arrived(weights.at[j, y2, low], w_ss.at[j, 0], w_rs.at[j, 3])

    def squares(c):
        for hh in range(2):
            for xx in range(4):
                have(c, slot(hh, xx, 1 - k))

        def body(i, _):
            rows = pl.ds(pl.multiple_of(i * 64, 64), 64)
            total = jnp.zeros((64, 128), F32)
            for s in range(16):
                v = acts[s, c, rows, :].astype(F32)
                v = v * v
                total = total + (v[:, :128] + v[:, 128:])
            sq[rows, :] = total
            return 0

        lax.fori_loop(0, 4, body, 0)
        for i in range(2):
            sq_own[c, i : i + 1, :] = jnp.sum(
                jnp.transpose(sq[i * 128 : (i + 1) * 128, :]), axis=0, keepdims=True
            )
        send(sq_own.at[c], sq_in.at[c], q_ss.at[c], q_rs.at[c], over)

    def norm(c):
        arrived(sq_in.at[c], q_ss.at[c], q_rs.at[c])
        for i in range(2):
            mean = (sq_own[c, i : i + 1, :] + sq_in[c, i : i + 1, :]) * (1.0 / 8192.0)
            inv[i * 128 : (i + 1) * 128, :] = jnp.transpose(
                jnp.broadcast_to(lax.rsqrt(mean + 1e-06), (128, 128))
            )

        def body(s, _):
            a, b, cc = s // 8, lax.rem(s // 2, 4), lax.rem(s, 2)
            at = pl.multiple_of(b * 1024 + (a * 2 + cc) * 256, 256)
            weight = gain[s * 2 + zl]
            for g in range(2):
                rows = pl.ds(g * PART, PART)
                scale = inv[rows, :]
                v = acts[s, c, rows, :].astype(F32)
                v = v * jnp.concatenate([scale, scale], axis=1) * weight
                normed[g, pl.ds(c * PART, PART), pl.ds(at, 256)] = v.astype(BF16)
            return 0

        lax.fori_loop(0, 16, body, 0)

    def project(g, j, first, count, out_ref):
        rows = pl.ds(first, count)

        def body(b, total):
            cols = pl.ds(pl.multiple_of(b * 1024, 1024), 1024)
            return total + jnp.dot(
                normed[g, rows, cols], weights[j, b], preferred_element_type=F32
            )

        out_ref[...] = lax.fori_loop(0, 4, body, jnp.zeros((count, HEAD), F32))

    own, other = zl, 1 - zl

    def give(j, n):
        project(other, j, n * BAND, BAND, psend.at[j, n])
        send(psend.at[j, n], precv.at[j, n], p_ss.at[j, n], p_rs.at[j, n], over)

    def keep(j):
        for n in range(2):
            project(own, j, n * 256, 256, kept_sum.at[j, pl.ds(n * 256, 256)])

    def result(j):
        for n in range(SPLIT):
            arrived(precv.at[j, n], p_ss.at[j, n], p_rs.at[j, n])
        return kept_sum[j] + precv[j].reshape(TOK, HEAD)

    def angles():
        for i in range(4):
            rows = slice(i * 128, (i + 1) * 128)
            at = jnp.transpose(jnp.broadcast_to(place[0, i : i + 1, :].astype(F32), (128, 128)))
            angle = at * frequency[...]
            lane = lax.broadcasted_iota(I32, (128, 128), 1)
            cosine[rows, :] = jnp.cos(angle)
            sine[rows, :] = jnp.where(lane < 64, -jnp.sin(angle), jnp.sin(angle))
            first_col[rows, :] = (
                lax.broadcasted_iota(I32, (128, 128), 0) + i * 128 - at.astype(I32)
            )

    def rotate(v):
        return v * cosine[...] + pltpu.roll(v, 64, axis=1) * sine[...]

    def first_row(n):
        return lax.broadcasted_iota(I32, (1, 128), 1) + n * 128 - place[0, n : n + 1, :]

    def attend(query, head):
        for block in range(2):
            seen = (block + 1) * 256
            rows = slice(block * 256, seen)
            scores = lax.dot_general(
                query[rows], kv[0, :seen, :], (((1,), (1,)), ((), ())), preferred_element_type=F32
            ) * (1.0 / HEAD**0.5)
            i = lax.broadcasted_iota(I32, (256, seen), 0) + block * 256
            j = lax.broadcasted_iota(I32, (256, seen), 1)
            starts = jnp.concatenate([first_col[rows, :]] * (seen // 128), axis=1)
            key_starts = jnp.concatenate([first_row(n) for n in range(seen // 128)], axis=1)
            allowed = (j <= i) & (starts == key_starts)
            scores = jnp.where(allowed, scores, NEG)
            largest = jnp.max(scores, axis=-1, keepdims=True)
            weight = jnp.where(allowed, jnp.exp(scores - largest), 0.0)
            probs = (weight / jnp.sum(weight, axis=-1, keepdims=True)).astype(BF16)
            out[rows, head * HEAD : (head + 1) * HEAD] = jnp.dot(
                probs, kv[1, :seen, :], preferred_element_type=F32
            ).astype(BF16)

    def keys():
        first = result(0)
        kv[k] = jnp.where(k == 0, rotate(first), first).astype(BF16)
        send(kv.at[k], kv.at[k], kv_ss, kv_rs, at_core)

    rows_a(0)
    rows_b(0)
    distribute_all()
    rows_a(1)
    rows_b(1)
    rows_own(0)
    rows_c(0)
    rows_own(1)
    rows_a(2)
    rows_own(2)
    rows_c(1)
    rows_b(2)
    finish_rows(0)
    rows_a(3)
    rows_own(3)
    rows_c(2)
    spread_own(0)
    finish_rows(1)
    rows_b(3)
    spread_near(0)
    spread_own(1)
    rows_c(3)
    angles()
    finish_rows(2)
    spread_far(0)
    weights_own(0)
    spread_near(1)
    weights_own(1)
    finish_rows(3)
    spread_pass(0)
    spread_own(2)
    spread_far(1)
    spread_own(3)
    weights_pass(0)
    spread_rest(0)
    spread_near(2)
    weights_own(2)
    squares(0)
    spread_far(2)
    spread_pass(1)
    weights_pass(1)
    norm(0)
    spread_near(3)
    spread_far(3)
    weights_own(3)
    spread_pass(2)
    spread_rest(1)
    weights_pass(2)
    spread_pass(3)
    squares(1)
    weights_own(4)
    spread_rest(2)
    norm(1)
    weights_whole(0)
    give(0, 0)
    weights_whole(1)
    give(1, 0)
    weights_pass(3)
    spread_rest(3)
    squares(2)
    weights_whole(2)
    give(2, 0)
    squares(3)
    norm(2)
    norm(3)
    give(0, 1)
    weights_pass(4)
    give(1, 1)
    give(2, 1)
    keep(0)
    weights_whole(3)
    give(3, 0)
    give(3, 1)
    keep(1)
    weights_whole(4)
    give(4, 0)
    give(4, 1)
    keys()
    keep(2)
    keep(3)
    keep(4)
    arrived(kv.at[1 - k], kv_ss, kv_rs)
    attend(rotate(result(1)).astype(BF16), 0)
    attend(rotate(result(2)).astype(BF16), 1)
    attend(rotate(result(3)).astype(BF16), 2)
    attend(rotate(result(4)).astype(BF16), 3)

    for copy in started:
        copy.wait_send()

    def settle(i, _):
        tt = lax.rem(t + i, 16)

        @pl.when(jnp.logical_not(jnp.logical_and(i == 0, plane == zl)))
        def _():
            for copy in outgoing(i, tt, wk):
                copy.wait_send()

        return 0

    lax.fori_loop(0, 16, settle, 0)


def on_device(token_ids, positions, embed_table, norm_gain, wq, wk, wv):
    frequency = 1000000.0 ** (-(jnp.arange(64, dtype=F32) * 2.0 / HEAD))
    vmem = pl.BlockSpec(memory_space=pltpu.VMEM)
    far = pl.BlockSpec(memory_space=pl.ANY)
    dma = pltpu.SemaphoreType.DMA
    return pl.pallas_call(
        kernel,
        out_shape=jax.ShapeDtypeStruct((TOK, 512), BF16),
        in_specs=[vmem] * 4 + [far] * 4,
        out_specs=vmem,
        scratch_shapes=[
            pltpu.VMEM((3, ROWS // TAB_COPIES, 512), BF16),
            pltpu.VMEM((ROWS + 8, 512), F32),
            pltpu.VMEM((PART, 512), F32),
            pltpu.VMEM((8, 4, 128), I32),
            pltpu.VMEM((8, 4, 128), I32),
            pltpu.SMEM((8, 4, 128), I32),
            pltpu.VMEM((CHUNKS, 4, 2, PART, 512), BF16),
            pltpu.VMEM((CHUNKS, 2, PART, 512), BF16),
            pltpu.VMEM((CHUNKS, 2, 2, PART, 512), BF16),
            pltpu.VMEM((CHUNKS, 2 * PART, 256), BF16),
            pltpu.VMEM((CHUNKS, 2 * PART, 256), BF16),
            pltpu.VMEM((16, CHUNKS, 2 * PART, 256), BF16),
            pltpu.VMEM((2, TOK, 4096), BF16),
            pltpu.VMEM((PIECES, 4, 1024, HEAD), BF16),
            pltpu.VMEM((PIECES, SPLIT, BAND, HEAD), F32),
            pltpu.VMEM((PIECES, SPLIT, BAND, HEAD), F32),
            pltpu.VMEM((PIECES, TOK, HEAD), F32),
            pltpu.VMEM((2, TOK, HEAD), BF16),
            pltpu.VMEM((2 * PART, 128), F32),
            pltpu.VMEM((CHUNKS, 2, 128), F32),
            pltpu.VMEM((CHUNKS, 2, 128), F32),
            pltpu.VMEM((2 * PART, 128), F32),
            pltpu.VMEM((TOK, 128), F32),
            pltpu.VMEM((TOK, 128), F32),
            pltpu.VMEM((TOK, 128), I32),
            dma((7,)), dma((7,)), dma((TAB_COPIES,)), dma,
            dma((16, PIECES)), dma((PIECES,)),
            dma((CHUNKS, 6)), dma((CHUNKS, 2)), dma((CHUNKS, 2, 2)),
            dma((CHUNKS,)), dma((CHUNKS,)),
            dma((CHUNKS, 15)), dma((CHUNKS, 16)),
            dma((CHUNKS,)), dma((CHUNKS,)),
            dma((PIECES, 4)), dma((PIECES, 4)),
            dma((PIECES, SPLIT)), dma((PIECES, SPLIT)),
            dma, dma,
        ],
        compiler_params=pltpu.CompilerParams(
            collective_id=0, has_side_effects=True, vmem_limit_bytes=63 * 2**20
        ),
    )(
        token_ids.reshape(1, 4, 128),
        positions.reshape(1, 4, 128),
        jnp.concatenate([frequency, frequency]).reshape(1, HEAD),
        norm_gain.reshape(32, 1, 256),
        embed_table,
        wq,
        wk,
        wv,
    )


def solution(mesh):
    split = P(("dp", "tensor"), None)
    return jax.shard_map(
        on_device,
        mesh=mesh,
        in_specs=(P("dp"), P("dp"), P("dp", "tensor"), P(), split, split, split),
        out_specs=P("dp", "tensor"),
        check_vma=False,
    )
```

```python
import jax
import jax.numpy as jnp
from jax import lax
from jax.experimental import pallas as pl
from jax.experimental.pallas import tpu as pltpu
from jax.sharding import PartitionSpec as P

MESH = pl.DeviceIdType.MESH
F32, BF16, I32 = jnp.float32, jnp.bfloat16, jnp.int32
TOK = 512
PART = 128
CHUNKS = TOK // PART
SPLIT = 2
BAND = TOK // SPLIT
PIECES = 5
ROWS = 9504
HEAD = 128
TAB_COPIES = 6
NEG = -1e30


def kernel(
    ids, place, frequency, gain, table, wq, wk, wv, out,
    landed, tab, stage, ids_all, index_v, index_s, mine, half_in, final_in,
    zsend, zrecv, acts, normed, weights, psend, precv, kept_sum, kv,
    sq, sq_own, sq_in, inv, cosine, sine, bias,
    ids_ss, ids_rs, tab_sem, sm_sem, x_ss, x_rs, g_ss, h_rs, f_rs, z_ss, z_rs,
    a_ss, a_rs, q_ss, q_rs, w_ss, w_rs, p_ss, p_rs, kv_ss, kv_rs,
):
    d = lax.axis_index("dp")
    t = lax.axis_index("tensor")
    zl, y = d // 4, lax.rem(d, 4)
    h, x, k = t // 8, lax.rem(t // 2, 4), lax.rem(t, 2)
    yp, y2, ym = lax.rem(y + 1, 4), lax.rem(y + 2, 4), lax.rem(y + 3, 4)
    xp, x2, xm = lax.rem(x + 1, 4), lax.rem(x + 2, 4), lax.rem(x + 3, 4)
    up, down, over = (zl * 4 + yp, t), (zl * 4 + ym, t), ((1 - zl) * 4 + y, t)

    def slot(hh, xx, kk):
        return hh * 8 + xx * 2 + kk

    started = []

    def send(src, dst, ss, rs, device):
        copy = pltpu.make_async_remote_copy(
            src_ref=src, dst_ref=dst, send_sem=ss, recv_sem=rs, device_id=device, device_id_type=MESH
        )
        copy.start()
        started.append(copy)

    def arrived(dst, ss, rs):
        pltpu.make_async_remote_copy(
            src_ref=dst, dst_ref=dst, send_sem=ss, recv_sem=rs, device_id=over, device_id_type=MESH
        ).wait_recv()

    part = ROWS // TAB_COPIES

    def load(i):
        return pltpu.make_async_copy(
            table.at[pl.ds(i * part, part)], landed.at[i % 3], tab_sem.at[i]
        )

    def widen(i):
        load(i).wait()

        def body(n, _):
            at = pl.multiple_of(n * 48, 16)
            tab[pl.ds(pl.multiple_of(i * part + n * 48, 16), 48), :] = landed[
                i % 3, pl.ds(at, 48), :
            ].astype(F32)
            return 0

        lax.fori_loop(0, part // 48, body, 0)
        if i + 3 < TAB_COPIES:
            load(i + 3).start()

    for i in range(3):
        load(i).start()

    barrier = pltpu.get_barrier_semaphore()

    def greet_plane(i, _):
        dd = lax.rem(zl + i // 16, 2) * 4 + y
        tt = lax.rem(t + i, 16)
        pl.semaphore_signal(barrier, inc=1, device_id=(dd, tt), device_id_type=MESH)
        return 0

    lax.fori_loop(1, 32, greet_plane, 0)

    def greet_row(i, _):
        dd = lax.rem(zl + i // 3, 2) * 4 + lax.rem(y + 1 + lax.rem(i, 3), 4)
        pl.semaphore_signal(barrier, inc=1, device_id=(dd, t), device_id_type=MESH)
        return 0

    lax.fori_loop(0, 6, greet_row, 0)
    pl.semaphore_wait(barrier, 37)

    for i in range(1, 8):
        send(ids.at[0], ids_all.at[d], ids_ss.at[i - 1], ids_rs.at[i - 1], (lax.rem(d + i, 8), t))

    tab[pl.ds(ROWS, 8), :] = jnp.zeros((8, 512), F32)
    for i in range(TAB_COPIES):
        widen(i)

    row = pl.multiple_of(((zl * 2 + h) * 4 + lax.rem(x, 2) * 2 + k) * 64, 64)
    plane = x // 2

    def pieces(tt, wkv):
        q0 = pl.multiple_of(tt * 512, 256)
        c0 = pl.multiple_of((tt // 2) * HEAD, HEAD)
        to = [weights.at[j, y, pl.ds(row, 64), :] for j in range(PIECES)]
        return [(wkv.at[:, pl.ds(c0, HEAD)], to[0], 0)] + [
            (wq.at[:, pl.ds(pl.multiple_of(q0 + n * HEAD, HEAD), HEAD)], to[n + 1], n + 1)
            for n in range(4)
        ]

    def outgoing(i, tt, wkv):
        return [
            pltpu.make_async_remote_copy(
                src_ref=src, dst_ref=dst, send_sem=x_ss.at[i, n], recv_sem=x_rs.at[r],
                device_id=(plane * 4 + y, tt), device_id_type=MESH,
            )
            for n, (src, dst, r) in enumerate(pieces(tt, wkv))
        ]

    def distribute(i, _):
        tt = lax.rem(t + i, 16)
        here = jnp.logical_and(i == 0, plane == zl)
        for core, wkv in ((0, wk), (1, wv)):
            turn = lax.rem(tt, 2) == core

            @pl.when(jnp.logical_and(turn, jnp.logical_not(here)))
            def _():
                for copy in outgoing(i, tt, wkv):
                    copy.start()

            @pl.when(jnp.logical_and(turn, here))
            def _():
                for src, dst, r in pieces(tt, wkv):
                    pltpu.make_async_copy(src, dst, x_rs.at[r]).start()

        return 0

    def distribute_all():
        lax.fori_loop(0, 16, distribute, 0)

    ids_all[d] = ids[0]
    for i in range(1, 8):
        arrived(ids_all.at[lax.rem(d + 8 - i, 8)], ids_ss.at[i - 1], ids_rs.at[i - 1])
    local = ids_all[...] - d * ROWS
    index_v[...] = jnp.where((local >= 0) & (local < ROWS), local, ROWS)
    to_scalar = pltpu.make_async_copy(index_v, index_s, sm_sem)
    to_scalar.start()
    to_scalar.wait()

    def gather(c, rel, g):
        group = g * 4 + lax.rem(y + rel, 4)

        def pick(i, _):
            for j in range(16):
                stage[pl.ds(i * 16 + j, 1), :] = tab[pl.ds(index_s[group, c, i * 16 + j], 1), :]
            return 0

        lax.fori_loop(0, PART // 16, pick, 0)

        def narrow(i, _):
            rows = pl.ds(pl.multiple_of(i * 64, 64), 64)
            mine[c, rel, g, rows, :] = stage[rows, :].astype(BF16)
            return 0

        lax.fori_loop(0, PART // 64, narrow, 0)

    def rows_a(c):
        for g, to in ((0, up), (1, down)):
            gather(c, 2, g)
            send(mine.at[c, 2, g], half_in.at[c, g], g_ss.at[c, g], h_rs.at[c, g], to)

    def rows_b(c):
        gather(c, 1, 1)
        send(mine.at[c, 1, 1], final_in.at[c, 0, 1], g_ss.at[c, 2], f_rs.at[c, 0, 1], up)
        gather(c, 3, 0)
        send(mine.at[c, 3, 0], final_in.at[c, 1, 0], g_ss.at[c, 3], f_rs.at[c, 1, 0], down)

    def rows_own(c):
        for rel, g in ((1, 0), (3, 1), (0, 0), (0, 1)):
            gather(c, rel, g)

    def rows_c(c):
        arrived(half_in.at[c, 0], g_ss.at[c, 0], h_rs.at[c, 0])
        mine[c, 1, 0] = mine[c, 1, 0] + half_in[c, 0]
        send(mine.at[c, 1, 0], final_in.at[c, 0, 0], g_ss.at[c, 4], f_rs.at[c, 0, 0], up)
        arrived(half_in.at[c, 1], g_ss.at[c, 1], h_rs.at[c, 1])
        mine[c, 3, 1] = mine[c, 3, 1] + half_in[c, 1]
        send(mine.at[c, 3, 1], final_in.at[c, 1, 1], g_ss.at[c, 5], f_rs.at[c, 1, 1], down)

    kept = pl.multiple_of(zl * 256, 256)
    given = pl.multiple_of((1 - zl) * 256, 256)

    def finish_rows(c):
        for g in range(2):
            for side in range(2):
                arrived(final_in.at[c, side, g], g_ss.at[c, 0], f_rs.at[c, side, g])
            rows = pl.ds(g * PART, PART)
            for at, to in ((given, None), (kept, t)):
                cols = pl.ds(at, 256)
                total = mine[c, 0, g, :, cols] + final_in[c, 0, g, :, cols] + final_in[c, 1, g, :, cols]
                if to is None:
                    zsend[c, rows, :] = total
                else:
                    acts[to, c, rows, :] = total
        send(zsend.at[c], zrecv.at[c], z_ss.at[c], z_rs.at[c], over)

    at_xp, at_xm = (d, slot(h, xp, k)), (d, slot(h, xm, k))
    at_z, at_core = (d, slot(1 - h, x, k)), (d, slot(h, x, 1 - k))

    def push(c, s, i, device):
        send(acts.at[s, c], acts.at[s, c], a_ss.at[c, i], a_rs.at[c, s], device)

    def have(c, s):
        arrived(acts.at[s, c], a_ss.at[c, 0], a_rs.at[c, s])

    def spread_own(c):
        arrived(zrecv.at[c], z_ss.at[c], z_rs.at[c])
        acts[t, c] = acts[t, c] + zrecv[c]
        push(c, t, 0, at_z)
        push(c, t, 1, at_xp)
        push(c, t, 2, at_xm)
        push(c, t, 3, at_core)

    def spread_near(c):
        s = slot(h, xm, k)
        have(c, s)
        push(c, s, 4, at_xp)
        push(c, s, 5, at_core)

    def spread_far(c):
        s = slot(1 - h, x, k)
        have(c, s)
        push(c, s, 7, at_xm)
        push(c, s, 8, at_xp)
        push(c, s, 9, at_core)

    def spread_pass(c):
        s = slot(1 - h, xp, k)
        have(c, s)
        push(c, s, 10, at_xm)
        push(c, s, 11, at_core)

    def spread_rest(c):
        for i, s in (
            (6, slot(h, xp, k)), (12, slot(1 - h, xm, k)), (13, slot(0, x2, k)), (14, slot(1, x2, k)),
        ):
            have(c, s)
            push(c, s, i, at_core)

    top, low = pl.ds(0, 512), pl.ds(512, 512)

    def weights_own(j):
        src = weights.at[j, y]
        pltpu.make_async_copy(src, src, x_rs.at[j]).wait()
        send(src, src, w_ss.at[j, 0], w_rs.at[j, 0], up)
        send(src, src, w_ss.at[j, 1], w_rs.at[j, 1], down)

    def weights_pass(j):
        arrived(weights.at[j, ym], w_ss.at[j, 0], w_rs.at[j, 0])
        src = weights.at[j, ym, top]
        send(src, src, w_ss.at[j, 2], w_rs.at[j, 2], up)
        arrived(weights.at[j, yp], w_ss.at[j, 0], w_rs.at[j, 1])
        src = weights.at[j, yp, low]
        send(src, src, w_ss.at[j, 3], w_rs.at[j, 3], down)

    def weights_whole(j):
        arrived(weights.at[j, y2, top], w_ss.at[j, 0], w_rs.at[j, 2])
        arrived(weights.at[j, y2, low], w_ss.at[j, 0], w_rs.at[j, 3])

    def squares(c):
        for hh in range(2):
            for xx in range(4):
                have(c, slot(hh, xx, 1 - k))

        def body(i, _):
            rows = pl.ds(pl.multiple_of(i * 64, 64), 64)
            total = jnp.zeros((64, 128), F32)
            for s in range(16):
                v = acts[s, c, rows, :].astype(F32)
                v = v * v
                total = total + (v[:, :128] + v[:, 128:])
            sq[rows, :] = total
            return 0

        lax.fori_loop(0, 4, body, 0)
        for i in range(2):
            sq_own[c, i : i + 1, :] = jnp.sum(
                jnp.transpose(sq[i * 128 : (i + 1) * 128, :]), axis=0, keepdims=True
            )
        send(sq_own.at[c], sq_in.at[c], q_ss.at[c], q_rs.at[c], over)

    def norm(c):
        arrived(sq_in.at[c], q_ss.at[c], q_rs.at[c])
        for i in range(2):
            mean = (sq_own[c, i : i + 1, :] + sq_in[c, i : i + 1, :]) * (1.0 / 8192.0)
            inv[i * 128 : (i + 1) * 128, :] = jnp.transpose(
                jnp.broadcast_to(lax.rsqrt(mean + 1e-06), (128, 128))
            )

        def body(s, _):
            a, b, cc = s // 8, lax.rem(s // 2, 4), lax.rem(s, 2)
            at = pl.multiple_of(b * 1024 + (a * 2 + cc) * 256, 256)
            weight = gain[s * 2 + zl]
            for g in range(2):
                rows = pl.ds(g * PART, PART)
                scale = inv[rows, :]
                v = acts[s, c, rows, :].astype(F32)
                v = v * jnp.concatenate([scale, scale], axis=1) * weight
                normed[g, pl.ds(c * PART, PART), pl.ds(at, 256)] = v.astype(BF16)
            return 0

        lax.fori_loop(0, 16, body, 0)

    def project(g, j, first, count, out_ref):
        rows = pl.ds(first, count)

        def body(b, total):
            cols = pl.ds(pl.multiple_of(b * 2048, 2048), 2048)
            w = weights[j, pl.ds(b * 2, 2)].reshape(2048, HEAD)
            return total + jnp.dot(normed[g, rows, cols], w, preferred_element_type=F32)

        out_ref[...] = lax.fori_loop(0, 2, body, jnp.zeros((count, HEAD), F32))

    own, other = zl, 1 - zl

    def give(j, n):
        project(other, j, n * BAND, BAND, psend.at[j, n])
        send(psend.at[j, n], precv.at[j, n], p_ss.at[j, n], p_rs.at[j, n], over)

    def keep(j, n):
        project(own, j, n * 256, 256, kept_sum.at[j, pl.ds(n * 256, 256)])

    def result(j):
        for n in range(SPLIT):
            arrived(precv.at[j, n], p_ss.at[j, n], p_rs.at[j, n])
        return kept_sum[j] + precv[j].reshape(TOK, HEAD)

    def angles():
        for i in range(4):
            rows = slice(i * 128, (i + 1) * 128)
            at = jnp.transpose(jnp.broadcast_to(place[0, i : i + 1, :].astype(F32), (128, 128)))
            angle = at * frequency[...]
            lane = lax.broadcasted_iota(I32, (128, 128), 1)
            cosine[rows, :] = jnp.cos(angle)
            sine[rows, :] = jnp.where(lane < 64, -jnp.sin(angle), jnp.sin(angle))
            row = lax.broadcasted_iota(I32, (128, 128), 0) + i * 128
            start = row - at.astype(I32)
            for n in range(i + 1):
                key = lane + n * 128
                seen = (key <= row) & (start == key - place[0, n : n + 1, :])
                bias[rows, n * 128 : (n + 1) * 128] = jnp.where(seen, 0.0, NEG)
            if i % 2 == 0:
                bias[rows, (i + 1) * 128 : (i + 2) * 128] = jnp.full((128, 128), NEG, F32)

    def rotate(v):
        return v * cosine[...] + pltpu.roll(v, 64, axis=1) * sine[...]

    def attend(query, head):
        for block in range(2):
            seen = (block + 1) * 256
            rows = slice(block * 256, seen)
            scores = lax.dot_general(
                query[rows], kv[0, :seen, :], (((1,), (1,)), ((), ())), preferred_element_type=F32
            ) * (1.0 / HEAD**0.5)
            scores = scores + bias[rows, :seen]
            largest = jnp.max(scores, axis=-1, keepdims=True)
            weight = jnp.exp(scores - largest)
            probs = (weight * (1.0 / jnp.sum(weight, axis=-1, keepdims=True))).astype(BF16)
            out[rows, head * HEAD : (head + 1) * HEAD] = jnp.dot(
                probs, kv[1, :seen, :], preferred_element_type=F32
            ).astype(BF16)

    def keys():
        first = result(0)
        kv[k] = jnp.where(k == 0, rotate(first), first).astype(BF16)
        send(kv.at[k], kv.at[k], kv_ss, kv_rs, at_core)

    rows_a(0)
    rows_b(0)
    distribute_all()
    rows_a(1)
    rows_b(1)
    rows_own(0)
    rows_c(0)
    rows_own(1)
    rows_a(2)
    rows_own(2)
    rows_c(1)
    rows_b(2)
    finish_rows(0)
    rows_a(3)
    rows_own(3)
    rows_c(2)
    spread_own(0)
    finish_rows(1)
    rows_b(3)
    spread_near(0)
    spread_own(1)
    rows_c(3)
    angles()
    finish_rows(2)
    spread_far(0)
    weights_own(0)
    spread_near(1)
    weights_own(1)
    finish_rows(3)
    spread_pass(0)
    spread_own(2)
    spread_far(1)
    spread_own(3)
    weights_pass(0)
    spread_rest(0)
    spread_near(2)
    weights_own(2)
    squares(0)
    spread_far(2)
    spread_pass(1)
    weights_pass(1)
    norm(0)
    spread_near(3)
    spread_far(3)
    weights_own(3)
    spread_pass(2)
    spread_rest(1)
    weights_pass(2)
    spread_pass(3)
    squares(1)
    weights_own(4)
    spread_rest(2)
    norm(1)
    weights_whole(0)
    give(0, 0)
    keep(0, 0)
    weights_whole(1)
    give(1, 0)
    keep(1, 0)
    weights_pass(3)
    spread_rest(3)
    squares(2)
    weights_whole(2)
    give(2, 0)
    squares(3)
    norm(2)
    norm(3)
    give(0, 1)
    weights_pass(4)
    give(1, 1)
    give(2, 1)
    keep(0, 1)
    weights_whole(3)
    give(3, 0)
    give(3, 1)
    keep(1, 1)
    weights_whole(4)
    give(4, 0)
    give(4, 1)
    keys()
    keep(2, 0)
    keep(2, 1)
    keep(3, 0)
    keep(3, 1)
    keep(4, 0)
    keep(4, 1)
    arrived(kv.at[1 - k], kv_ss, kv_rs)
    attend(rotate(result(1)).astype(BF16), 0)
    attend(rotate(result(2)).astype(BF16), 1)
    attend(rotate(result(3)).astype(BF16), 2)
    attend(rotate(result(4)).astype(BF16), 3)

    for copy in started:
        copy.wait_send()

    def settle(i, _):
        tt = lax.rem(t + i, 16)

        @pl.when(jnp.logical_not(jnp.logical_and(i == 0, plane == zl)))
        def _():
            for copy in outgoing(i, tt, wk):
                copy.wait_send()

        return 0

    lax.fori_loop(0, 16, settle, 0)


def on_device(token_ids, positions, embed_table, norm_gain, wq, wk, wv):
    frequency = 1000000.0 ** (-(jnp.arange(64, dtype=F32) * 2.0 / HEAD))
    vmem = pl.BlockSpec(memory_space=pltpu.VMEM)
    far = pl.BlockSpec(memory_space=pl.ANY)
    dma = pltpu.SemaphoreType.DMA
    return pl.pallas_call(
        kernel,
        out_shape=jax.ShapeDtypeStruct((TOK, 512), BF16),
        in_specs=[vmem] * 4 + [far] * 4,
        out_specs=vmem,
        scratch_shapes=[
            pltpu.VMEM((3, ROWS // TAB_COPIES, 512), BF16),
            pltpu.VMEM((ROWS + 8, 512), F32),
            pltpu.VMEM((PART, 512), F32),
            pltpu.VMEM((8, 4, 128), I32),
            pltpu.VMEM((8, 4, 128), I32),
            pltpu.SMEM((8, 4, 128), I32),
            pltpu.VMEM((CHUNKS, 4, 2, PART, 512), BF16),
            pltpu.VMEM((CHUNKS, 2, PART, 512), BF16),
            pltpu.VMEM((CHUNKS, 2, 2, PART, 512), BF16),
            pltpu.VMEM((CHUNKS, 2 * PART, 256), BF16),
            pltpu.VMEM((CHUNKS, 2 * PART, 256), BF16),
            pltpu.VMEM((16, CHUNKS, 2 * PART, 256), BF16),
            pltpu.VMEM((2, TOK, 4096), BF16),
            pltpu.VMEM((PIECES, 4, 1024, HEAD), BF16),
            pltpu.VMEM((PIECES, SPLIT, BAND, HEAD), F32),
            pltpu.VMEM((PIECES, SPLIT, BAND, HEAD), F32),
            pltpu.VMEM((PIECES, TOK, HEAD), F32),
            pltpu.VMEM((2, TOK, HEAD), BF16),
            pltpu.VMEM((2 * PART, 128), F32),
            pltpu.VMEM((CHUNKS, 2, 128), F32),
            pltpu.VMEM((CHUNKS, 2, 128), F32),
            pltpu.VMEM((2 * PART, 128), F32),
            pltpu.VMEM((TOK, 128), F32),
            pltpu.VMEM((TOK, 128), F32),
            pltpu.VMEM((TOK, TOK), F32),
            dma((7,)), dma((7,)), dma((TAB_COPIES,)), dma,
            dma((16, PIECES)), dma((PIECES,)),
            dma((CHUNKS, 6)), dma((CHUNKS, 2)), dma((CHUNKS, 2, 2)),
            dma((CHUNKS,)), dma((CHUNKS,)),
            dma((CHUNKS, 15)), dma((CHUNKS, 16)),
            dma((CHUNKS,)), dma((CHUNKS,)),
            dma((PIECES, 4)), dma((PIECES, 4)),
            dma((PIECES, SPLIT)), dma((PIECES, SPLIT)),
            dma, dma,
        ],
        compiler_params=pltpu.CompilerParams(
            collective_id=0, has_side_effects=True, vmem_limit_bytes=63 * 2**20
        ),
    )(
        token_ids.reshape(1, 4, 128),
        positions.reshape(1, 4, 128),
        jnp.concatenate([frequency, frequency]).reshape(1, HEAD),
        norm_gain.reshape(32, 1, 256),
        embed_table,
        wq,
        wk,
        wv,
    )


def solution(mesh):
    split = P(("dp", "tensor"), None)
    return jax.shard_map(
        on_device,
        mesh=mesh,
        in_specs=(P("dp"), P("dp"), P("dp", "tensor"), P(), split, split, split),
        out_specs=P("dp", "tensor"),
        check_vma=False,
    )
```
